256 devices in a mesh: rep: 1, dp: 256 (over x, y, z, core).
Axes of the slice: x: 4, y: 4, z: 8, core: 2. Of those that a mesh axis runs over, the one named last changes fastest.
Arguments:
- x: bfloat16 [256, 1024, 1024], P(('rep', 'dp'))
- dy: bfloat16 [256, 1024, 1024], P(('rep', 'dp'))
- w_gate: bfloat16 [2, 1024, 2816], replicated
- w_up: bfloat16 [2, 1024, 2816], replicated
- w_down: bfloat16 [2, 2816, 1024], replicated
- m_w_gate: float32 [2, 1024, 2816], replicated
- m_w_up: float32 [2, 1024, 2816], replicated
- m_w_down: float32 [2, 2816, 1024], replicated
- v_w_gate: float32 [2, 1024, 2816], replicated
- v_w_up: float32 [2, 1024, 2816], replicated
- v_w_down: float32 [2, 2816, 1024], replicated
Outputs:
- output 1: bfloat16 [2, 1024, 2816], P('rep')
- output 2: bfloat16 [2, 1024, 2816], P('rep')
- output 3: bfloat16 [2, 2816, 1024], P('rep')
- output 4: float32 [2, 1024, 2816], P('rep')
- output 5: float32 [2, 1024, 2816], P('rep')
- output 6: float32 [2, 2816, 1024], P('rep')
- output 7: float32 [2, 1024, 2816], P('rep')
- output 8: float32 [2, 1024, 2816], P('rep')
- output 9: float32 [2, 2816, 1024], P('rep')
All inputs are finite; a program needn't handle non-finite values.
Results may differ from the reference program's by a relative error of at most 0.022.
Values are sent between devices in bfloat16 or wider.
A program may use at most 768 MiB of HBM per device.

```python
import jax
import jax.numpy as jnp
from jax import lax

SEQUENCES = 256
TOKENS = 1024
D = 1024
FF = 2816
LAYERS = 2
NAMES = ("w_gate", "w_up", "w_down")
SHAPES = {"w_gate": (LAYERS, D, FF), "w_up": (LAYERS, D, FF), "w_down": (LAYERS, FF, D)}


def bump(key, n, height):
    away = (jnp.arange(n, dtype=jnp.int32) - jax.random.randint(key, (), 0, n, jnp.int32)) % n
    return jnp.where(away < n // 8, height, 1.0)


def together(key, own, strength):
    shared = jax.random.normal(key, own.shape[1:], jnp.float32)
    return (own + strength * shared) * lax.rsqrt(1 + strength * strength)


def setup_inputs(seed: int = 0, part: int = 0) -> dict:
    kx, kdy, ka, kb, kz, kf, kh, kl, *keys = jax.random.split(jax.random.key(seed), 8 + 3 * len(NAMES))
    kx, kdy, ka, kb = (jax.random.fold_in(k, part) for k in (kx, kdy, ka, kb))
    kw, km, kv = (keys[i::3] for i in range(3))
    shape = (SEQUENCES, TOKENS, D)
    much_x, much_dy = jax.random.uniform(kz, (2,), jnp.float32, 0.0, 1.0)
    loud = 2.0 ** jax.random.uniform(jax.random.fold_in(kz, 1), (), jnp.float32, -1.0, 2.0)
    layers = 2.0 ** jax.random.uniform(kl, (LAYERS, 1, 1), jnp.float32, -1.0, 1.0)
    x = together(ka, jax.random.normal(kx, shape, jnp.float32), much_x) * bump(kf, D, 4.0)
    dy = together(kb, jax.random.normal(kdy, shape, jnp.float32), much_dy)
    drawn = {"x": x.astype(jnp.bfloat16), "dy": (loud * dy * (SEQUENCES * TOKENS) ** -0.5).astype(jnp.bfloat16)}
    for key, name in zip(kw, NAMES, strict=True):
        w = jax.random.normal(key, SHAPES[name], jnp.float32) * SHAPES[name][1] ** -0.5
        drawn[name] = (w * {"w_gate": 1.0, "w_up": bump(kh, FF, 4.0), "w_down": layers}[name]).astype(jnp.bfloat16)
    for key, name in zip(km, NAMES, strict=True):
        drawn[f"m_{name}"] = 0.1 * jax.random.normal(key, SHAPES[name], jnp.float32)
    for key, name in zip(kv, NAMES, strict=True):
        drawn[f"v_{name}"] = loud * loud * jax.random.uniform(key, SHAPES[name], jnp.float32, 0.05, 0.15)
    return drawn


def matmul(a, w):
    return jnp.dot(a, w, preferred_element_type=jnp.float32).astype(jnp.bfloat16)


def normed(h):
    wide = h.astype(jnp.float32)
    scale = lax.rsqrt(jnp.mean(wide**2, -1, keepdims=True) + 1e-6)
    return (wide * scale).astype(jnp.bfloat16)


def layer(h, w):
    a = normed(h)
    gate = jnp.dot(a, w["w_gate"], preferred_element_type=jnp.float32)
    up = jnp.dot(a, w["w_up"], preferred_element_type=jnp.float32)
    return h + matmul((jax.nn.silu(gate) * up).astype(jnp.bfloat16), w["w_down"])


def adamw(w, m, v, g):
    m = 0.9 * m + 0.1 * g
    v = 0.95 * v + 0.05 * g * g
    step = m * lax.rsqrt(v + 1e-8) + 0.1 * w
    return (w - 0.02 * step).astype(jnp.bfloat16), m, v


def stack(weights, h):
    return lax.scan(lambda h, w: (layer(h, w), None), h, weights)[0]


def reference(x, dy, w_gate, w_up, w_down, m_w_gate, m_w_up, m_w_down, v_w_gate, v_w_up, v_w_down):
    weights = dict(zip(NAMES, (w_gate, w_up, w_down), strict=True))

    def take(so_far, sequence):
        h, by_y = sequence
        _, back = jax.vjp(lambda w: stack(w, h), weights)
        return jax.tree.map(lambda total, term: total + term.astype(jnp.float32), so_far, back(by_y)[0]), None

    none_yet = {name: jnp.zeros(w.shape, jnp.float32) for name, w in weights.items()}
    by_weights, _ = lax.scan(take, none_yet, (x, dy))
    gradients = [by_weights[name].astype(jnp.bfloat16).astype(jnp.float32) for name in NAMES]
    new = [
        adamw(w.astype(jnp.float32), m, v, g)
        for w, m, v, g in zip((w_gate, w_up, w_down), (m_w_gate, m_w_up, m_w_down), (v_w_gate, v_w_up, v_w_down), gradients, strict=True)
    ]
    return tuple(one[which] for which in range(3) for one in new)
```

```python
import functools

import jax
import jax.numpy as jnp
from jax import lax
from jax.experimental import pallas as pl
from jax.experimental.pallas import tpu as pltpu
from jax.sharding import PartitionSpec as P

MESH = pl.DeviceIdType.MESH

SIZE = {"x": 4, "y": 4, "z": 8}
TILES = 2816
HALF = TILES // 2
COLORS = []
_start = 0
for _axes, _unit, _first in (("xyz", 4, 2), ("yxz", 4, 2), ("zxy", 3, 0)):
    _n3 = _unit
    _n2 = _n3 * SIZE[_axes[2]]
    _n1 = _n2 * SIZE[_axes[1]]
    COLORS.append((_axes, _start, (_n1, _n2, _n3), _first))
    _start += _n1 * SIZE[_axes[0]]
assert _start == HALF
MATRICES = 6
BATCH = 3
LAG = 3


def ring_slots(n, hops):
    slots, at = [], 0
    for hop in range(hops):
        row = []
        for way in range(2):
            first = n - n // 2 if way == 0 else n // 2
            size = first if hop == 0 else n
            row.append((at, size))
            at += size
        slots.append(row)
    return slots, at


class Layout:
    def __init__(self):
        self.r1, self.r2, self.r3, self.s3, self.fin = [], [], [], [], []
        a1 = a2 = a3 = s3 = fin = 0
        self.sem = {}
        for c, (axes, _, (n1, n2, n3), _) in enumerate(COLORS):
            h1, h2, k3 = SIZE[axes[0]] // 2, SIZE[axes[1]] // 2, SIZE[axes[2]]
            slots, size = ring_slots(n1, h1)
            self.r1.append([[(a1 + s, n) for s, n in row] for row in slots])
            a1 += size
            slots, size = ring_slots(n2, h2)
            self.r2.append([[(a2 + s, n) for s, n in row] for row in slots])
            a2 += size
            self.r3.append(a3)
            a3 += (k3 - 1) * n3
            self.s3.append(s3)
            s3 += n2
            self.fin.append(fin)
            fin += n3
            for kind, count in (("r1", 2 * h1), ("r2", 2 * h2), ("r3", 1), ("g3", 1), ("g2", 2 * h2), ("g1", 2 * h1)):
                self.sem[c, kind] = len(self.sem_list) if hasattr(self, "sem_list") else 0
                if not hasattr(self, "sem_list"):
                    self.sem_list = []
                self.sem[c, kind] = len(self.sem_list)
                self.sem_list += [kind] * count
        self.n1, self.n2, self.n3, self.ns, self.nf = a1, a2, a3, s3, fin
        self.sems = len(self.sem_list)


LAY = Layout()


def out_index(m):
    return m % BATCH * 2 + (1 - m // BATCH)


def add_tiles(dst, dst_at, size, terms, chunk=8):
    def some(at, n):
        total = None
        for ref, start in terms:
            value = ref[pl.ds(start + at, n)].astype(jnp.float32)
            total = value if total is None else total + value
        dst[pl.ds(dst_at + at, n)] = total.astype(jnp.bfloat16)

    full = size // chunk
    if full > 1:
        lax.fori_loop(0, full, lambda i, _: (some(i * chunk, chunk), 0)[1], 0)
    elif full == 1:
        some(0, chunk)
    if size % chunk:
        some(full * chunk, size % chunk)


def reduce_kernel(*refs):
    grads, (out, own, par, r1, r2, r3, s3, fin, send_rs, send_ag, recv, pair, load) = refs[:MATRICES], refs[MATRICES:]
    me = lax.axis_index("dp")
    core = me % 2
    place = {"x": me // 64, "y": me // 16 % 4, "z": me // 2 % 8}

    def device(axis=None, by=0):
        at = dict(place)
        c = core
        if axis is None:
            c = 1 - core
        else:
            at[axis] = (at[axis] + by) % SIZE[axis]
        return (0, ((at["x"] * 4 + at["y"]) * 8 + at["z"]) * 2 + c)

    barrier = pltpu.get_barrier_semaphore()
    peers = [device()] + [device("x", 1), device("x", -1)] + [device("y", d) for d in (1, 2, 3)] + [device("z", d) for d in range(1, 8)]
    for peer in peers:
        pl.semaphore_signal(barrier, inc=1, device_id=peer, device_id_type=MESH)

    mine, theirs = core * HALF, (1 - core) * HALF

    def remote(src, dst, send, receive, to):
        return pltpu.make_async_remote_copy(
            src_ref=src, dst_ref=dst, send_sem=send, recv_sem=receive, device_id=to, device_id_type=MESH
        )

    def arrived(ref, n, sem):
        pltpu.make_async_copy(ref.at[pl.ds(0, n)], ref.at[pl.ds(0, n)], sem).wait()

    for m in range(MATRICES):
        pltpu.make_async_copy(grads[m].at[pl.ds(mine, HALF)], own.at[m], load.at[m, 0]).start()
    pl.semaphore_wait(barrier, len(peers))
    for m in range(MATRICES):
        remote(grads[m].at[pl.ds(theirs, HALF)], par.at[m], send_rs.at[m], pair.at[m, 0], device()).start()

    def sem(m, c, kind, i=0):
        return recv.at[m, LAY.sem[c, kind] + i]

    def color_stage(c, stage, m):
        axes, start, (n1, n2, n3), _ = COLORS[c]
        k1, k2, k3 = (SIZE[a] for a in axes)
        p1, p2, p3 = (place[a] for a in axes)
        h1, h2 = k1 // 2, k2 // 2
        o, q, a1, a2, a3 = own.at[m], par.at[m], r1.at[m], r2.at[m], r3.at[m]
        result = out.at[out_index(m)]
        base2 = start + p1 * n1
        base3 = base2 + p2 * n2
        shard = base3 + p3 * n3

        def ring_reduce(axis, k, p, n, base, hop, slots, arrivals, kind, more):
            h = k // 2
            j = h - hop
            for way, sign in ((0, 1), (1, -1)):
                owner = (p + sign * j) % k
                at = base + owner * n
                lo, size = (0, n) if j < h else ((0, n - n // 2) if way == 0 else (n - n // 2, n // 2))
                extra = [(ref, where + owner * n) for ref, where in more]
                if hop == 0:
                    add_tiles(o, at + lo, size, [(o, at + lo), (q, at + lo)] + [(r, w + lo) for r, w in extra])
                else:
                    there, got = slots[hop - 1][way]
                    arrived(arrivals, got, sem(m, c, kind, 2 * (hop - 1) + way))
                    if got == n:
                        add_tiles(o, at, n, [(o, at), (q, at)] + extra + [(arrivals, there)])
                    else:
                        first = 0 if way == 0 else n - got
                        add_tiles(o, at + first, got, [(o, at + first), (q, at + first)] + [(r, w + first) for r, w in extra] + [(arrivals, there)])
                        other, rest = (got, n - got) if way == 0 else (0, n - got)
                        add_tiles(o, at + other, rest, [(o, at + other), (q, at + other)] + [(r, w + other) for r, w in extra])
                there, size2 = slots[hop][way]
                assert size2 == size
                remote(
                    o.at[pl.ds(at + lo, size)], arrivals.at[pl.ds(there, size)], send_rs.at[m], sem(m, c, kind, 2 * hop + way), device(axis, sign)
                ).start()

        def ring_wait(k, slots, arrivals, kind):
            h = k // 2
            for way in range(2):
                arrived(arrivals, slots[h - 1][way][1], sem(m, c, kind, 2 * (h - 1) + way))

        def gather_sizes(k, n, hop):
            h = k // 2
            return [(0, n), (0, n)] if hop < h - 1 else [(0, n - n // 2), (n - n // 2, n // 2)]

        def gather_wait(k, n, hop, kind):
            for way in range(2):
                arrived(result, gather_sizes(k, n, hop)[way][1], sem(m, c, kind, 2 * hop + way))

        def ring_gather(axis, k, p, n, base, hop, kind):
            if hop:
                gather_wait(k, n, hop - 1, kind)
            for way, sign in ((0, 1), (1, -1)):
                lo, size = gather_sizes(k, n, hop)[way]
                at = mine + base + (p - sign * hop) % k * n + lo
                piece = result.at[pl.ds(at, size)]
                remote(piece, piece, send_ag.at[m], sem(m, c, kind, 2 * hop + way), device(axis, sign)).start()

        last1 = [(a1, LAY.r1[c][h1 - 1][way][0]) for way in range(2)]
        last2 = [(a2, LAY.r2[c][h2 - 1][way][0]) for way in range(2)]
        if stage < h1:
            ring_reduce(axes[0], k1, p1, n1, start, stage, LAY.r1[c], a1, "r1", [])
            return
        stage -= h1
        if stage < h2:
            if stage == 0:
                ring_wait(k1, LAY.r1[c], a1, "r1")
            ring_reduce(axes[1], k2, p2, n2, base2, stage, LAY.r2[c], a2, "r2", last1)
            return
        stage -= h2
        if stage == 0:
            ring_wait(k2, LAY.r2[c], a2, "r2")
            add_tiles(s3.at[m], LAY.s3[c], n2, [(o, base3), (q, base3)] + [(r, w + p2 * n2) for r, w in last1] + last2)
            for d in range(1, k3):
                owner = (p3 + d) % k3
                remote(
                    s3.at[m, pl.ds(LAY.s3[c] + owner * n3, n3)],
                    a3.at[pl.ds(LAY.r3[c] + (d - 1) * n3, n3)],
                    send_rs.at[m],
                    sem(m, c, "r3"),
                    device(axes[2], d),
                ).start()
            return
        stage -= 1
        if stage == 0:
            arrived(a3, (k3 - 1) * n3, sem(m, c, "r3"))
            terms = [(o, shard), (q, shard)] + [(r, w + p2 * n2 + p3 * n3) for r, w in last1] + [(r, w + p3 * n3) for r, w in last2]
            terms += [(a3, LAY.r3[c] + (d - 1) * n3) for d in range(1, k3)]
            add_tiles(fin.at[m], LAY.fin[c], n3, terms)
            piece = fin.at[m, pl.ds(LAY.fin[c], n3)]
            place_of = result.at[pl.ds(mine + shard, n3)]
            pltpu.make_async_copy(piece, place_of, load.at[m, 1 + c]).start()
            for d in range(1, k3):
                remote(piece, place_of, send_ag.at[m], sem(m, c, "g3"), device(axes[2], d)).start()
            return
        stage -= 1
        if stage < h2:
            if stage == 0:
                arrived(result, n3, load.at[m, 1 + c])
                arrived(result, (k3 - 1) * n3, sem(m, c, "g3"))
            ring_gather(axes[1], k2, p2, n2, base2, stage, "g2")
            return
        stage -= h2
        if stage < h1:
            if stage == 0:
                gather_wait(k2, n2, h2 - 1, "g2")
            ring_gather(axes[0], k1, p1, n1, start, stage, "g1")
            return
        stage -= h1
        if stage == 0:
            gather_wait(k1, n1, h1 - 1, "g1")

    def stages_of(c):
        axes = COLORS[c][0]
        return 2 * (SIZE[axes[0]] // 2 + SIZE[axes[1]] // 2) + 3

    ends = max(COLORS[c][3] + stages_of(c) for c in range(3))

    def slot(s, m):
        result = out.at[out_index(m)]
        if s == 0:
            arrived(own.at[m], HALF, load.at[m, 0])
            arrived(par.at[m], HALF, pair.at[m, 0])
        for c in (2, 0, 1):
            i = s - COLORS[c][3]
            if 0 <= i < stages_of(c):
                color_stage(c, i, m)
        if s == ends:
            half = result.at[pl.ds(mine, HALF)]
            remote(half, half, send_ag.at[m], pair.at[m, 1], device()).start()

    for s in range(ends + 1 + LAG):
        for batch in range(2):
            i = s - batch * LAG
            if 0 <= i <= ends:
                lax.fori_loop(batch * BATCH, (batch + 1) * BATCH, lambda m, _: (slot(i, m), 0)[1], 0)

    sent = HALF + LAY.n1 + LAY.n2 + LAY.n3

    def finish(m, _):
        result = out.at[out_index(m)]
        arrived(result, HALF, pair.at[m, 1])
        arrived(result, sent, send_rs.at[m])
        arrived(result, sent, send_ag.at[m])
        return 0

    lax.fori_loop(0, MATRICES, finish, 0)


def reduce_gradients(grads):
    tiles = lambda *n: pltpu.VMEM((MATRICES, *n, 8, 128), jnp.bfloat16)
    dma = pltpu.SemaphoreType.DMA
    return pl.pallas_call(
        reduce_kernel,
        out_shape=jax.ShapeDtypeStruct((MATRICES, TILES, 8, 128), jnp.bfloat16),
        in_specs=[pl.BlockSpec(memory_space=pl.ANY)] * MATRICES,
        out_specs=pl.BlockSpec(memory_space=pl.ANY),
        scratch_shapes=[
            tiles(HALF), tiles(HALF), tiles(LAY.n1), tiles(LAY.n2), tiles(LAY.n3), tiles(LAY.ns), tiles(LAY.nf),
            dma((MATRICES,)), dma((MATRICES,)), dma((MATRICES, LAY.sems)), dma((MATRICES, 2)), dma((MATRICES, 4)),
        ],
        compiler_params=pltpu.CompilerParams(collective_id=0, has_side_effects=True, vmem_limit_bytes=58 * 2**20),
        name="reduce_gradients",
    )(*grads)


NAMES = ("w_gate", "w_up", "w_down")

def matmul(a, w):
    return jnp.dot(a, w, preferred_element_type=jnp.float32).astype(jnp.bfloat16)


def normed(h):
    wide = h.astype(jnp.float32)
    scale = lax.rsqrt(jnp.mean(wide**2, -1, keepdims=True) + 1e-6)
    return (wide * scale).astype(jnp.bfloat16)


def layer(h, w):
    a = normed(h)
    gate = jnp.dot(a, w["w_gate"], preferred_element_type=jnp.float32)
    up = jnp.dot(a, w["w_up"], preferred_element_type=jnp.float32)
    return h + matmul((jax.nn.silu(gate) * up).astype(jnp.bfloat16), w["w_down"])


def adamw_kernel(w, m, v, g, new_w, new_m, new_v):
    g = g[0].astype(jnp.float32)
    m = 0.9 * m[...] + 0.1 * g
    v = 0.95 * v[...] + 0.05 * g * g
    w = w[...].astype(jnp.float32)
    step = m * lax.rsqrt(v + 1e-8) + 0.1 * w
    new_w[...] = (w - 0.02 * step).astype(jnp.bfloat16)
    new_m[...] = m
    new_v[...] = v


def adamw(which, w, m, v, g, block=176):
    spec = pl.BlockSpec((block, 8, 128), lambda i: (i, 0, 0))
    return pl.pallas_call(
        adamw_kernel,
        out_shape=[jax.ShapeDtypeStruct(a.shape, a.dtype) for a in (w, m, v)],
        grid=(w.shape[0] // block,),
        in_specs=[spec, spec, spec, pl.BlockSpec((1, block, 8, 128), lambda i: (which, i, 0, 0))],
        out_specs=[spec] * 3,
        name="adamw",
    )(w, m, v, g)


def to_tiles(a):
    *lead, rows, columns = a.shape
    a = a.reshape(*lead, rows // 8, 8, columns // 128, 128)
    return jnp.swapaxes(a, -3, -2).reshape(-1, 8, 128)


def from_tiles(t, shape):
    *lead, rows, columns = shape
    t = t.reshape(*lead, rows // 8, columns // 128, 8, 128)
    return jnp.swapaxes(t, -3, -2).reshape(shape)


def solution(mesh):
    def step(x, dy, *arrays):
        weights, m, v = (arrays[i : i + 3] for i in (0, 3, 6))
        layers = weights[0].shape[0]
        h, kept = x[0], []
        for number in range(layers):
            kept.append(h)
            h = layer(h, {name: w[number] for name, w in zip(NAMES, weights, strict=True)})
        by_h, terms = dy[0], []
        for number in reversed(range(layers)):
            _, back = jax.vjp(lambda w, h: layer(h, w), {name: w[number] for name, w in zip(NAMES, weights, strict=True)}, kept[number])
            by_w, by_h = back(by_h)
            terms += [to_tiles(by_w[name]) for name in NAMES]
        summed = reduce_gradients(terms).reshape(3, layers * TILES, 8, 128)
        new = [adamw(i, to_tiles(w), to_tiles(m), to_tiles(v), summed) for i, (w, m, v) in enumerate(zip(weights, m, v, strict=True))]
        return tuple(from_tiles(one[which], w.shape) for which in range(3) for one, w in zip(new, weights, strict=True))

    return jax.shard_map(
        step,
        mesh=mesh,
        in_specs=(P(("rep", "dp"), None, None),) * 2 + (P(None, None, None),) * 9,
        out_specs=(P("rep", None, None),) * 9,
        check_vma=False,
    )
```

```python
import functools

import jax
import jax.numpy as jnp
from jax import lax
from jax.experimental import pallas as pl
from jax.experimental.pallas import tpu as pltpu
from jax.sharding import PartitionSpec as P

MESH = pl.DeviceIdType.MESH

SIZE = {"x": 4, "y": 4, "z": 8}
TILES = 2816
HALF = TILES // 2
COLORS = []
_start = 0
for _axes, _unit, _first in (("xyz", 4, 2), ("yxz", 4, 2), ("zxy", 3, 0)):
    _n3 = _unit
    _n2 = _n3 * SIZE[_axes[2]]
    _n1 = _n2 * SIZE[_axes[1]]
    COLORS.append((_axes, _start, (_n1, _n2, _n3), _first))
    _start += _n1 * SIZE[_axes[0]]
assert _start == HALF
MATRICES = 6
BATCH = 3
LAG = 3


def ring_slots(n, hops):
    slots, at = [], 0
    for hop in range(hops):
        row = []
        for way in range(2):
            first = n - n // 2 if way == 0 else n // 2
            size = first if hop == 0 else n
            row.append((at, size))
            at += size
        slots.append(row)
    return slots, at


class Layout:
    def __init__(self):
        self.r1, self.r2, self.r3, self.s3, self.fin = [], [], [], [], []
        a1 = a2 = a3 = s3 = fin = 0
        self.sem = {}
        for c, (axes, _, (n1, n2, n3), _) in enumerate(COLORS):
            h1, h2, k3 = SIZE[axes[0]] // 2, SIZE[axes[1]] // 2, SIZE[axes[2]]
            slots, size = ring_slots(n1, h1)
            self.r1.append([[(a1 + s, n) for s, n in row] for row in slots])
            a1 += size
            slots, size = ring_slots(n2, h2)
            self.r2.append([[(a2 + s, n) for s, n in row] for row in slots])
            a2 += size
            self.r3.append(a3)
            a3 += (k3 - 1) * n3
            self.s3.append(s3)
            s3 += n2
            self.fin.append(fin)
            fin += n3
            for kind, count in (("r1", 2 * h1), ("r2", 2 * h2), ("r3", 1), ("g3", 1), ("g2", 2 * h2), ("g1", 2 * h1)):
                self.sem[c, kind] = len(self.sem_list) if hasattr(self, "sem_list") else 0
                if not hasattr(self, "sem_list"):
                    self.sem_list = []
                self.sem[c, kind] = len(self.sem_list)
                self.sem_list += [kind] * count
        self.n1, self.n2, self.n3, self.ns, self.nf = a1, a2, a3, s3, fin
        self.sems = len(self.sem_list)


LAY = Layout()


def out_index(m):
    return m % BATCH * 2 + (1 - m // BATCH)


def add_tiles(dst, dst_at, size, terms, chunk=8):
    def some(at, n):
        total = None
        for ref, start in terms:
            value = ref[pl.ds(start + at, n)].astype(jnp.float32)
            total = value if total is None else total + value
        dst[pl.ds(dst_at + at, n)] = total.astype(jnp.bfloat16)

    full = size // chunk
    if full > 1:
        lax.fori_loop(0, full, lambda i, _: (some(i * chunk, chunk), 0)[1], 0)
    elif full == 1:
        some(0, chunk)
    if size % chunk:
        some(full * chunk, size % chunk)


def reduce_kernel(*refs):
    grads, (out, own, par, r1, r2, r3, s3, fin, send_rs, send_ag, recv, pair, load) = refs[:MATRICES], refs[MATRICES:]
    me = lax.axis_index("dp")
    core = me % 2
    place = {"x": me // 64, "y": me // 16 % 4, "z": me // 2 % 8}

    def device(axis=None, by=0):
        at = dict(place)
        c = core
        if axis is None:
            c = 1 - core
        else:
            at[axis] = (at[axis] + by) % SIZE[axis]
        return (0, ((at["x"] * 4 + at["y"]) * 8 + at["z"]) * 2 + c)

    barrier = pltpu.get_barrier_semaphore()
    peers = [device()] + [device("x", 1), device("x", -1)] + [device("y", d) for d in (1, 2, 3)] + [device("z", d) for d in range(1, 8)]
    for peer in peers:
        pl.semaphore_signal(barrier, inc=1, device_id=peer, device_id_type=MESH)

    mine, theirs = core * HALF, (1 - core) * HALF

    def remote(src, dst, send, receive, to):
        return pltpu.make_async_remote_copy(
            src_ref=src, dst_ref=dst, send_sem=send, recv_sem=receive, device_id=to, device_id_type=MESH
        )

    def arrived(ref, n, sem):
        pltpu.make_async_copy(ref.at[pl.ds(0, n)], ref.at[pl.ds(0, n)], sem).wait()

    for m in range(MATRICES):
        pltpu.make_async_copy(grads[m].at[pl.ds(mine, HALF)], own.at[m], load.at[m, 0]).start()
    pl.semaphore_wait(barrier, len(peers))
    for m in range(MATRICES):
        remote(grads[m].at[pl.ds(theirs, HALF)], par.at[m], send_rs.at[m], pair.at[m, 0], device()).start()

    def sem(m, c, kind, i=0):
        return recv.at[m, LAY.sem[c, kind] + i]

    def color_stage(c, stage, m):
        axes, start, (n1, n2, n3), _ = COLORS[c]
        k1, k2, k3 = (SIZE[a] for a in axes)
        p1, p2, p3 = (place[a] for a in axes)
        h1, h2 = k1 // 2, k2 // 2
        o, q, a1, a2, a3 = own.at[m], par.at[m], r1.at[m], r2.at[m], r3.at[m]
        result = out.at[out_index(m)]
        base2 = start + p1 * n1
        base3 = base2 + p2 * n2
        shard = base3 + p3 * n3

        def ring_reduce(axis, k, p, n, base, hop, slots, arrivals, kind, more):
            h = k // 2
            j = h - hop
            for way, sign in ((0, 1), (1, -1)):
                owner = (p + sign * j) % k
                at = base + owner * n
                lo, size = (0, n) if j < h else ((0, n - n // 2) if way == 0 else (n - n // 2, n // 2))
                extra = [(ref, where + owner * n) for ref, where in more]
                if hop == 0:
                    add_tiles(o, at + lo, size, [(o, at + lo), (q, at + lo)] + [(r, w + lo) for r, w in extra])
                else:
                    there, got = slots[hop - 1][way]
                    arrived(arrivals, got, sem(m, c, kind, 2 * (hop - 1) + way))
                    if got == n:
                        add_tiles(o, at, n, [(o, at), (q, at)] + extra + [(arrivals, there)])
                    else:
                        first = 0 if way == 0 else n - got
                        add_tiles(o, at + first, got, [(o, at + first), (q, at + first)] + [(r, w + first) for r, w in extra] + [(arrivals, there)])
                        other, rest = (got, n - got) if way == 0 else (0, n - got)
                        add_tiles(o, at + other, rest, [(o, at + other), (q, at + other)] + [(r, w + other) for r, w in extra])
                there, size2 = slots[hop][way]
                assert size2 == size
                remote(
                    o.at[pl.ds(at + lo, size)], arrivals.at[pl.ds(there, size)], send_rs.at[m], sem(m, c, kind, 2 * hop + way), device(axis, sign)
                ).start()

        def ring_wait(k, slots, arrivals, kind):
            h = k // 2
            for way in range(2):
                arrived(arrivals, slots[h - 1][way][1], sem(m, c, kind, 2 * (h - 1) + way))

        def gather_sizes(k, n, hop):
            h = k // 2
            return [(0, n), (0, n)] if hop < h - 1 else [(0, n - n // 2), (n - n // 2, n // 2)]

        def gather_wait(k, n, hop, kind):
            for way in range(2):
                arrived(result, gather_sizes(k, n, hop)[way][1], sem(m, c, kind, 2 * hop + way))

        def ring_gather(axis, k, p, n, base, hop, kind):
            if hop:
                gather_wait(k, n, hop - 1, kind)
            for way, sign in ((0, 1), (1, -1)):
                lo, size = gather_sizes(k, n, hop)[way]
                at = mine + base + (p - sign * hop) % k * n + lo
                piece = result.at[pl.ds(at, size)]
                remote(piece, piece, send_ag.at[m], sem(m, c, kind, 2 * hop + way), device(axis, sign)).start()

        last1 = [(a1, LAY.r1[c][h1 - 1][way][0]) for way in range(2)]
        last2 = [(a2, LAY.r2[c][h2 - 1][way][0]) for way in range(2)]
        if stage < h1:
            ring_reduce(axes[0], k1, p1, n1, start, stage, LAY.r1[c], a1, "r1", [])
            return
        stage -= h1
        if stage < h2:
            if stage == 0:
                ring_wait(k1, LAY.r1[c], a1, "r1")
            ring_reduce(axes[1], k2, p2, n2, base2, stage, LAY.r2[c], a2, "r2", last1)
            return
        stage -= h2
        if stage == 0:
            ring_wait(k2, LAY.r2[c], a2, "r2")
            add_tiles(s3.at[m], LAY.s3[c], n2, [(o, base3), (q, base3)] + [(r, w + p2 * n2) for r, w in last1] + last2)
            for d in range(1, k3):
                owner = (p3 + d) % k3
                remote(
                    s3.at[m, pl.ds(LAY.s3[c] + owner * n3, n3)],
                    a3.at[pl.ds(LAY.r3[c] + (d - 1) * n3, n3)],
                    send_rs.at[m],
                    sem(m, c, "r3"),
                    device(axes[2], d),
                ).start()
            return
        stage -= 1
        if stage == 0:
            arrived(a3, (k3 - 1) * n3, sem(m, c, "r3"))
            terms = [(o, shard), (q, shard)] + [(r, w + p2 * n2 + p3 * n3) for r, w in last1] + [(r, w + p3 * n3) for r, w in last2]
            terms += [(a3, LAY.r3[c] + (d - 1) * n3) for d in range(1, k3)]
            add_tiles(fin.at[m], LAY.fin[c], n3, terms)
            piece = fin.at[m, pl.ds(LAY.fin[c], n3)]
            place_of = result.at[pl.ds(mine + shard, n3)]
            pltpu.make_async_copy(piece, place_of, load.at[m, 1 + c]).start()
            for d in range(1, k3):
                remote(piece, place_of, send_ag.at[m], sem(m, c, "g3"), device(axes[2], d)).start()
            return
        stage -= 1
        if stage < h2:
            if stage == 0:
                arrived(result, n3, load.at[m, 1 + c])
                arrived(result, (k3 - 1) * n3, sem(m, c, "g3"))
            ring_gather(axes[1], k2, p2, n2, base2, stage, "g2")
            return
        stage -= h2
        if stage < h1:
            if stage == 0:
                gather_wait(k2, n2, h2 - 1, "g2")
            ring_gather(axes[0], k1, p1, n1, start, stage, "g1")
            return
        stage -= h1
        if stage == 0:
            gather_wait(k1, n1, h1 - 1, "g1")

    def stages_of(c):
        axes = COLORS[c][0]
        return 2 * (SIZE[axes[0]] // 2 + SIZE[axes[1]] // 2) + 3

    ends = max(COLORS[c][3] + stages_of(c) for c in range(3))

    def slot(s, m):
        result = out.at[out_index(m)]
        if s == 0:
            arrived(own.at[m], HALF, load.at[m, 0])
            arrived(par.at[m], HALF, pair.at[m, 0])
        for c in (2, 0, 1):
            i = s - COLORS[c][3]
            if 0 <= i < stages_of(c):
                color_stage(c, i, m)
        if s == ends:
            half = result.at[pl.ds(mine, HALF)]
            remote(half, half, send_ag.at[m], pair.at[m, 1], device()).start()

    for s in range(ends + 1 + LAG):
        for batch in range(2):
            i = s - batch * LAG
            if 0 <= i <= ends:
                lax.fori_loop(batch * BATCH, (batch + 1) * BATCH, lambda m, _: (slot(i, m), 0)[1], 0)

    sent = HALF + LAY.n1 + LAY.n2 + LAY.n3

    def finish(m, _):
        result = out.at[out_index(m)]
        arrived(result, HALF, pair.at[m, 1])
        arrived(result, sent, send_rs.at[m])
        arrived(result, sent, send_ag.at[m])
        return 0

    lax.fori_loop(0, MATRICES, finish, 0)


def reduce_gradients(grads):
    tiles = lambda *n: pltpu.VMEM((MATRICES, *n, 8, 128), jnp.bfloat16)
    dma = pltpu.SemaphoreType.DMA
    return pl.pallas_call(
        reduce_kernel,
        out_shape=jax.ShapeDtypeStruct((MATRICES, TILES, 8, 128), jnp.bfloat16),
        in_specs=[pl.BlockSpec(memory_space=pl.ANY)] * MATRICES,
        out_specs=pl.BlockSpec(memory_space=pl.ANY),
        scratch_shapes=[
            tiles(HALF), tiles(HALF), tiles(LAY.n1), tiles(LAY.n2), tiles(LAY.n3), tiles(LAY.ns), tiles(LAY.nf),
            dma((MATRICES,)), dma((MATRICES,)), dma((MATRICES, LAY.sems)), dma((MATRICES, 2)), dma((MATRICES, 4)),
        ],
        compiler_params=pltpu.CompilerParams(collective_id=0, has_side_effects=True, vmem_limit_bytes=58 * 2**20),
        name="reduce_gradients",
    )(*grads)


FF_BLOCK = 256


def dot(a, b, contract=(1, 0)):
    return lax.dot_general(a, b, (((contract[0],), (contract[1],)), ((), ())), preferred_element_type=jnp.float32)


ROWS = 128


def by_rows(total, body):
    lax.fori_loop(0, total // ROWS, lambda i, _: (body(pl.ds(pl.multiple_of(i * ROWS, ROWS), ROWS)), 0)[1], 0)


def norm_rows(h, a, tokens):
    def some(rows):
        wide = h[0, rows, :].astype(jnp.float32)
        scale = lax.rsqrt(jnp.mean(wide**2, -1, keepdims=True) + 1e-6)
        a[rows, :] = (wide * scale).astype(jnp.bfloat16)

    by_rows(tokens, some)


def forward_kernel(h, w_gate, w_up, w_down, gate_out, up_out, h_out, a, total):
    step = pl.program_id(0)
    tokens = a.shape[0]

    @pl.when(step == 0)
    def _():
        norm_rows(h, a, tokens)

    gate = dot(a[...], w_gate[0])
    up = dot(a[...], w_up[0])
    gate_out[...] = gate
    up_out[...] = up
    hidden = (gate * jax.nn.sigmoid(gate) * up).astype(jnp.bfloat16)
    part = dot(hidden, w_down[0])

    @pl.when(step == 0)
    def _():
        total[...] = part

    @pl.when(step > 0)
    def _():
        total[...] += part

    @pl.when(step == pl.num_programs(0) - 1)
    def _():
        def some(rows):
            h_out[0, rows, :] = (h[0, rows, :].astype(jnp.float32) + total[rows, :].astype(jnp.bfloat16).astype(jnp.float32)).astype(jnp.bfloat16)

        by_rows(tokens, some)


def hidden_backward(gate, up, by_hidden):
    s = jax.nn.sigmoid(gate)
    act = gate * s
    by_hidden = by_hidden.astype(jnp.bfloat16).astype(jnp.float32)
    hidden = (act * up).astype(jnp.bfloat16)
    by_up = (by_hidden * act).astype(jnp.bfloat16)
    by_gate = (by_hidden * up * (s * (1 + gate * (1 - s)))).astype(jnp.bfloat16)
    return hidden, by_gate, by_up


def last_layer_kernel(h, dy, w_gate, w_up, w_down, g_gate, g_up, g_down, h_out, a, a_t, total):
    step = pl.program_id(0)
    tokens = a.shape[0]

    @pl.when(step == 0)
    def _():
        norm_rows(h, a, tokens)
        a_t[...] = a[...].T

    gate = dot(a[...], w_gate[0])
    up = dot(a[...], w_up[0])
    by_hidden = dot(dy[0], w_down[0], (1, 1))
    hidden, by_gate, by_up = hidden_backward(gate, up, by_hidden)
    g_down[...] = dot(hidden, dy[0], (0, 0)).astype(jnp.bfloat16)
    g_gate[...] = dot(a_t[...], by_gate).astype(jnp.bfloat16)
    g_up[...] = dot(a_t[...], by_up).astype(jnp.bfloat16)
    part = dot(by_gate, w_gate[0], (1, 1)) + dot(by_up, w_up[0], (1, 1))

    @pl.when(step == 0)
    def _():
        total[...] = part

    @pl.when(step > 0)
    def _():
        total[...] += part

    @pl.when(step == pl.num_programs(0) - 1)
    def _():
        width = a.shape[1]

        def some(rows):
            wide = h[0, rows, :].astype(jnp.float32)
            by_a = total[rows, :].astype(jnp.bfloat16).astype(jnp.float32)
            scale = lax.rsqrt(jnp.mean(wide**2, -1, keepdims=True) + 1e-6)
            along = jnp.sum(by_a * wide, -1, keepdims=True)
            by_wide = by_a * scale - wide * (scale * scale * scale * along * (1.0 / width))
            h_out[0, rows, :] = (dy[0, rows, :].astype(jnp.float32) + by_wide.astype(jnp.bfloat16).astype(jnp.float32)).astype(jnp.bfloat16)

        by_rows(tokens, some)


def first_layer_kernel(h, by_h, gate, up, w_down, g_gate, g_up, g_down, a, a_t):
    @pl.when(pl.program_id(0) == 0)
    def _():
        norm_rows(h, a, a.shape[0])
        a_t[...] = a[...].T

    by_hidden = dot(by_h[0], w_down[0], (1, 1))
    hidden, by_gate, by_up = hidden_backward(gate[...], up[...], by_hidden)
    g_down[...] = dot(hidden, by_h[0], (0, 0)).astype(jnp.bfloat16)
    g_gate[...] = dot(a_t[...], by_gate).astype(jnp.bfloat16)
    g_up[...] = dot(a_t[...], by_up).astype(jnp.bfloat16)


def forward_and_backward(x, dy, w_gate, w_up, w_down):
    _, tokens, d = x.shape
    ff = w_gate.shape[2]
    block = FF_BLOCK
    grid = (ff // block,)
    whole = pl.BlockSpec((1, tokens, d), lambda i: (0, 0, 0), pipeline_mode=pl.Buffered(1))
    wide = lambda n: pl.BlockSpec((1, d, block), lambda i: (n, 0, i))
    tall = lambda n: pl.BlockSpec((1, block, d), lambda i: (n, i, 0))
    hidden = pl.BlockSpec((tokens, block), lambda i: (0, i))
    g_specs = [pl.BlockSpec((d, block), lambda i: (0, i))] * 2 + [pl.BlockSpec((block, d), lambda i: (i, 0))]
    bf, f32 = jnp.bfloat16, jnp.float32
    g_shapes = [jax.ShapeDtypeStruct((d, ff), bf)] * 2 + [jax.ShapeDtypeStruct((ff, d), bf)]
    states = pltpu.VMEM((tokens, d), bf)
    turned = pltpu.VMEM((d, tokens), bf)
    sums = pltpu.VMEM((tokens, d), f32)
    params = pltpu.CompilerParams(vmem_limit_bytes=56 * 2**20)
    gate, up, h = pl.pallas_call(
        forward_kernel,
        out_shape=[jax.ShapeDtypeStruct((tokens, ff), f32)] * 2 + [jax.ShapeDtypeStruct(x.shape, bf)],
        grid=grid,
        in_specs=[whole, wide(0), wide(0), tall(0)],
        out_specs=[hidden, hidden, whole],
        scratch_shapes=[states, sums],
        compiler_params=params,
        name="first_layer_forward",
    )(x, w_gate, w_up, w_down)
    *last, by_h = pl.pallas_call(
        last_layer_kernel,
        out_shape=g_shapes + [jax.ShapeDtypeStruct(x.shape, bf)],
        grid=grid,
        in_specs=[whole, whole, wide(1), wide(1), tall(1)],
        out_specs=g_specs + [whole],
        scratch_shapes=[states, turned, sums],
        compiler_params=params,
        name="last_layer",
    )(h, dy, w_gate, w_up, w_down)
    first = pl.pallas_call(
        first_layer_kernel,
        out_shape=g_shapes,
        grid=grid,
        in_specs=[whole, whole, hidden, hidden, tall(0)],
        out_specs=g_specs,
        scratch_shapes=[states, turned],
        compiler_params=params,
        name="first_layer_backward",
    )(x, by_h, gate, up, w_down)
    return [*last, *first]


def adamw_kernel(w, m, v, g, new_w, new_m, new_v):
    g = g[0].astype(jnp.float32)
    m = 0.9 * m[...] + 0.1 * g
    v = 0.95 * v[...] + 0.05 * g * g
    w = w[...].astype(jnp.float32)
    step = m * lax.rsqrt(v + 1e-8) + 0.1 * w
    new_w[...] = (w - 0.02 * step).astype(jnp.bfloat16)
    new_m[...] = m
    new_v[...] = v


def adamw(which, w, m, v, g, block=704):
    spec = pl.BlockSpec((block, 8, 128), lambda i: (i, 0, 0))
    return pl.pallas_call(
        adamw_kernel,
        out_shape=[jax.ShapeDtypeStruct(a.shape, a.dtype) for a in (w, m, v)],
        grid=(w.shape[0] // block,),
        in_specs=[spec, spec, spec, pl.BlockSpec((1, block, 8, 128), lambda i: (which, i, 0, 0))],
        out_specs=[spec] * 3,
        compiler_params=pltpu.CompilerParams(vmem_limit_bytes=56 * 2**20),
        name="adamw",
    )(w, m, v, g)


def to_tiles(a):
    *lead, rows, columns = a.shape
    a = a.reshape(*lead, rows // 8, 8, columns // 128, 128)
    return jnp.swapaxes(a, -3, -2).reshape(-1, 8, 128)


def from_tiles(t, shape):
    *lead, rows, columns = shape
    t = t.reshape(*lead, rows // 8, columns // 128, 8, 128)
    return jnp.swapaxes(t, -3, -2).reshape(shape)


def solution(mesh):
    def step(x, dy, *arrays):
        weights, m, v = (arrays[i : i + 3] for i in (0, 3, 6))
        terms = [to_tiles(g) for g in forward_and_backward(x, dy, *weights)]
        summed = reduce_gradients(terms).reshape(3, 2 * TILES, 8, 128)
        new = [adamw(i, to_tiles(w), to_tiles(m), to_tiles(v), summed) for i, (w, m, v) in enumerate(zip(weights, m, v, strict=True))]
        return tuple(from_tiles(one[which], w.shape) for which in range(3) for one, w in zip(new, weights, strict=True))

    return jax.shard_map(
        step,
        mesh=mesh,
        in_specs=(P(("rep", "dp"), None, None),) * 2 + (P(None, None, None),) * 9,
        out_specs=(P("rep", None, None),) * 9,
        check_vma=False,
    )
```

```python
import jax
import jax.numpy as jnp
from jax import lax
from jax.experimental import pallas as pl
from jax.experimental.pallas import tpu as pltpu
from jax.sharding import PartitionSpec as P

MESH = pl.DeviceIdType.MESH
BF16, F32 = jnp.bfloat16, jnp.float32

BLOCK = 256
BLOCKS = 11
UNITS = 11
HALF = 768
SIZE = {"x": 4, "y": 4, "z": 8}
COLORS = []
_start = 0
_rings = [0, 2, 4, 5, 6, 7, 8, 9, 10, 12, 14]
for _axes, _slots in (("xyz", _rings), ("yxz", _rings), ("zxy", list(range(15)))):
    _n3 = 2
    _n2 = _n3 * SIZE[_axes[2]]
    _n1 = _n2 * SIZE[_axes[1]]
    COLORS.append((_axes, _start, (_n1, _n2, _n3), _slots))
    _start += _n1 * SIZE[_axes[0]]
assert _start == HALF
FIN_SLOT, SWAP_SLOT, END_SLOT = 7, 15, 16
HELD = 6
PACE = 3
LAST_CALLS, FIRST_CALLS = 4, 2
COMPUTE_CALLS = BLOCKS * (LAST_CALLS + FIRST_CALLS)


def ready(m):
    return jnp.where(m < 5, 8 * m + 8, jnp.where(m == 5, 46, 4 * m + 26))


CALLS = COMPUTE_CALLS + PACE * (END_SLOT + 1) + 1


def ring_slots(n, hops):
    slots, at = [], 0
    for hop in range(hops):
        row = []
        for way in range(2):
            first = n - n // 2 if way == 0 else n // 2
            size = first if hop == 0 else n
            row.append((at, size))
            at += size
        slots.append(row)
    return slots, at


class Layout:
    def __init__(self):
        self.r1, self.r2, self.r3, self.s3, self.fin, self.sem = [], [], [], [], [], {}
        a1 = a2 = a3 = s3 = fin = sems = 0
        for c, (axes, _, (n1, n2, n3), _) in enumerate(COLORS):
            h1, h2, k3 = SIZE[axes[0]] // 2, SIZE[axes[1]] // 2, SIZE[axes[2]]
            slots, size = ring_slots(n1, h1)
            self.r1.append([[(a1 + s, n) for s, n in row] for row in slots])
            a1 += size
            slots, size = ring_slots(n2, h2)
            self.r2.append([[(a2 + s, n) for s, n in row] for row in slots])
            a2 += size
            self.r3.append(a3)
            a3 += (k3 - 1) * n3
            self.s3.append(s3)
            s3 += n2
            self.fin.append(fin)
            fin += n3
            for kind, count in (("r1", 2 * h1), ("r2", 2 * h2), ("r3", 1), ("g3", 1), ("g2", 2 * h2), ("g1", 2 * h1)):
                self.sem[c, kind] = sems
                sems += count
        self.n1, self.n2, self.n3, self.ns, self.nf, self.sems = a1, a2, a3, s3, fin, sems


LAY = Layout()
SENT = HALF + LAY.n1 + LAY.n2 + LAY.n3


def add_tiles(dst, dst_at, size, terms, chunk=8):
    def some(at, n):
        total = None
        for ref, start in terms:
            value = ref[pl.ds(start + at, n)].astype(F32)
            total = value if total is None else total + value
        dst[pl.ds(dst_at + at, n)] = total.astype(BF16)

    full = size // chunk
    if full > 1:
        lax.fori_loop(0, full, lambda i, _: (some(i * chunk, chunk), 0)[1], 0)
    elif full == 1:
        some(0, chunk)
    if size % chunk:
        some(full * chunk, size % chunk)


def remote(src, dst, send, receive, to):
    return pltpu.make_async_remote_copy(src_ref=src, dst_ref=dst, send_sem=send, recv_sem=receive, device_id=to, device_id_type=MESH)


def arrived(ref, n, sem):
    pltpu.make_async_copy(ref.at[pl.ds(0, n)], ref.at[pl.ds(0, n)], sem).wait()


class Engine:
    def __init__(self, terms, out, own, par, r1, r2, r3, s3, fin, send_rs, send_ag, recv, pair, load, written, credit):
        self.terms, self.out, self.own, self.par, self.r1, self.r2, self.r3, self.s3, self.fin = terms, out, own, par, r1, r2, r3, s3, fin
        self.send_rs, self.send_ag, self.recv, self.pair, self.load, self.written, self.credit = send_rs, send_ag, recv, pair, load, written, credit
        me = lax.axis_index("dp")
        self.core = me % 2
        self.place = {"x": me // 64, "y": me // 16 % 4, "z": me // 2 % 8}
        self.peers = [self.device()] + [self.device("x", d) for d in (1, 3)]
        self.peers += [self.device("y", d) for d in (1, 2, 3)] + [self.device("z", d) for d in range(1, 8)]

    def device(self, axis=None, by=0):
        at = dict(self.place)
        core = self.core
        if axis is None:
            core = 1 - core
        else:
            at[axis] = (at[axis] + by + SIZE[axis]) % SIZE[axis]
        return (0, ((at["x"] * 4 + at["y"]) * 8 + at["z"]) * 2 + core)

    def greet(self):
        for peer in self.peers:
            pl.semaphore_signal(pltpu.get_barrier_semaphore(), inc=1, device_id=peer, device_id_type=MESH)

    def meet(self):
        pl.semaphore_wait(pltpu.get_barrier_semaphore(), len(self.peers))

    def begin(self, m):
        for half in range(2):
            arrived(self.out.at[0], HALF, self.written.at[half])

        @pl.when(m >= HELD)
        def _():
            pl.semaphore_wait(self.credit.at[m - HELD], len(self.peers))
            arrived(self.out.at[0], SENT, self.send_rs.at[m - HELD])

        unit = pl.ds(m * HALF, HALF)
        pltpu.make_async_copy(self.terms.at[self.core, unit], self.own.at[m % HELD], self.load.at[m, 0]).start()
        remote(self.terms.at[1 - self.core, unit], self.par.at[m % HELD], self.send_rs.at[m], self.pair.at[m, 0], self.device()).start()

    def color_stage(self, c, stage, m):
        axes, start, (n1, n2, n3), _ = COLORS[c]
        k1, k2, k3 = (SIZE[a] for a in axes)
        p1, p2, p3 = (self.place[a] for a in axes)
        h1, h2 = k1 // 2, k2 // 2
        b = m % HELD
        o, q, a1, a2, a3 = (ref.at[b] for ref in (self.own, self.par, self.r1, self.r2, self.r3))
        result, mine = self.out.at[self.core], m * HALF
        send_rs, send_ag, load = self.send_rs.at[m], self.send_ag.at[m], self.load.at[m, 1 + c]
        device = self.device
        base2 = start + p1 * n1
        base3 = base2 + p2 * n2
        shard = base3 + p3 * n3

        def sem(kind, i=0):
            return self.recv.at[m, LAY.sem[c, kind] + i]

        def ring_reduce(axis, k, p, n, base, hop, slots, arrivals, kind, more):
            h = k // 2
            j = h - hop
            for way, sign in ((0, 1), (1, -1)):
                owner = (p + sign * j + k) % k
                at = base + owner * n
                lo, size = (0, n) if j < h else ((0, n - n // 2) if way == 0 else (n - n // 2, n // 2))
                extra = [(ref, where + owner * n) for ref, where in more]
                if hop == 0:
                    add_tiles(o, at + lo, size, [(o, at + lo), (q, at + lo)] + [(r, w + lo) for r, w in extra])
                else:
                    there, got = slots[hop - 1][way]
                    arrived(arrivals, got, sem(kind, 2 * (hop - 1) + way))
                    if got == n:
                        add_tiles(o, at, n, [(o, at), (q, at)] + extra + [(arrivals, there)])
                    else:
                        first = 0 if way == 0 else n - got
                        add_tiles(o, at + first, got, [(o, at + first), (q, at + first)] + [(r, w + first) for r, w in extra] + [(arrivals, there)])
                        other, rest = (got, n - got) if way == 0 else (0, n - got)
                        add_tiles(o, at + other, rest, [(o, at + other), (q, at + other)] + [(r, w + other) for r, w in extra])
                there, size2 = slots[hop][way]
                assert size2 == size
                remote(o.at[pl.ds(at + lo, size)], arrivals.at[pl.ds(there, size)], send_rs, sem(kind, 2 * hop + way), device(axis, sign)).start()

        def ring_wait(h, slots, arrivals, kind):
            for way in range(2):
                arrived(arrivals, slots[h - 1][way][1], sem(kind, 2 * (h - 1) + way))

        def gather_sizes(k, n, hop):
            return [(0, n), (0, n)] if hop < k // 2 - 1 else [(0, n - n // 2), (n - n // 2, n // 2)]

        def gather_wait(k, n, hop, kind):
            for way in range(2):
                arrived(result, gather_sizes(k, n, hop)[way][1], sem(kind, 2 * hop + way))

        def ring_gather(axis, k, p, n, base, hop, kind):
            if hop:
                gather_wait(k, n, hop - 1, kind)
            for way, sign in ((0, 1), (1, -1)):
                lo, size = gather_sizes(k, n, hop)[way]
                piece = result.at[pl.ds(mine + base + (p - sign * hop + k) % k * n + lo, size)]
                remote(piece, piece, send_ag, sem(kind, 2 * hop + way), device(axis, sign)).start()

        last1 = [(a1, LAY.r1[c][h1 - 1][way][0]) for way in range(2)]
        last2 = [(a2, LAY.r2[c][h2 - 1][way][0]) for way in range(2)]
        if stage < h1:
            ring_reduce(axes[0], k1, p1, n1, start, stage, LAY.r1[c], a1, "r1", [])
            return
        stage -= h1
        if stage < h2:
            if stage == 0:
                ring_wait(h1, LAY.r1[c], a1, "r1")
            ring_reduce(axes[1], k2, p2, n2, base2, stage, LAY.r2[c], a2, "r2", last1)
            return
        stage -= h2
        if stage == 0:
            ring_wait(h2, LAY.r2[c], a2, "r2")
            add_tiles(self.s3.at[b], LAY.s3[c], n2, [(o, base3), (q, base3)] + [(r, w + p2 * n2) for r, w in last1] + last2)
            for d in range(1, k3):
                piece = self.s3.at[b, pl.ds(LAY.s3[c] + (p3 + d) % k3 * n3, n3)]
                remote(piece, a3.at[pl.ds(LAY.r3[c] + (d - 1) * n3, n3)], send_rs, sem("r3"), device(axes[2], d)).start()
            return
        stage -= 1
        if stage == 0:
            arrived(a3, (k3 - 1) * n3, sem("r3"))
            terms = [(o, shard), (q, shard)] + [(r, w + p2 * n2 + p3 * n3) for r, w in last1] + [(r, w + p3 * n3) for r, w in last2]
            terms += [(a3, LAY.r3[c] + (d - 1) * n3) for d in range(1, k3)]
            add_tiles(self.fin.at[m], LAY.fin[c], n3, terms)
            piece = self.fin.at[m, pl.ds(LAY.fin[c], n3)]
            there = result.at[pl.ds(mine + shard, n3)]
            pltpu.make_async_copy(piece, there, load).start()
            for d in range(1, k3):
                remote(piece, there, send_ag, sem("g3"), device(axes[2], d)).start()
            return
        stage -= 1
        if stage < h2:
            if stage == 0:
                arrived(result, n3, load)
                arrived(result, (k3 - 1) * n3, sem("g3"))
            ring_gather(axes[1], k2, p2, n2, base2, stage, "g2")
            return
        stage -= h2
        if stage < h1:
            if stage == 0:
                gather_wait(k2, n2, h2 - 1, "g2")
            ring_gather(axes[0], k1, p1, n1, start, stage, "g1")
            return
        gather_wait(k1, n1, h1 - 1, "g1")

    def slot(self, s, m):
        if s == -1:
            self.begin(m)
        if s == 0:
            arrived(self.out.at[0], HALF, self.load.at[m, 0])
            arrived(self.out.at[0], HALF, self.pair.at[m, 0])
        for c in (2, 0, 1):
            if s in COLORS[c][3]:
                self.color_stage(c, COLORS[c][3].index(s), m)
        if s == FIN_SLOT:

            @pl.when(m < UNITS - HELD)
            def _():
                for peer in self.peers:
                    pl.semaphore_signal(self.credit.at[m], inc=1, device_id=peer, device_id_type=MESH)

        if s == SWAP_SLOT:
            piece = self.out.at[self.core, pl.ds(m * HALF, HALF)]
            remote(piece, piece, self.send_ag.at[m], self.pair.at[m, 1], self.device()).start()
        if s == END_SLOT:
            arrived(self.out.at[0], HALF, self.pair.at[m, 1])
            arrived(self.out.at[0], SENT, self.send_ag.at[m])

    def step(self, call):
        def unit(m, _):
            since = call - ready(m)

            @pl.when((since >= 0) & (since <= PACE * (END_SLOT + 1)) & (since % PACE == 0))
            def _():
                s = since // PACE - 1
                for low in range(-1, END_SLOT + 1, 3):

                    @pl.when((s >= low) & (s < low + 3))
                    def _():
                        for one in range(low, min(low + 3, END_SLOT + 1)):
                            pl.when(s == one)(lambda one=one: self.slot(one, m))

            return 0

        lax.fori_loop(0, UNITS, unit, 0)

    def finish(self):
        def unit(m, _):
            arrived(self.out.at[0], SENT, self.send_rs.at[m])
            return 0

        lax.fori_loop(UNITS - HELD, UNITS, unit, 0)


def dot(a, b, contract=(1, 0)):
    return lax.dot_general(a, b, (((contract[0],), (contract[1],)), ((), ())), preferred_element_type=F32)


ROWS = 128


def by_rows(total, body):
    lax.fori_loop(0, total // ROWS, lambda i, _: (body(pl.ds(pl.multiple_of(i * ROWS, ROWS), ROWS)), 0)[1], 0)


def norm_rows(h, a):
    def some(rows):
        wide = h[0, rows, :].astype(F32)
        scale = lax.rsqrt(jnp.mean(wide**2, -1, keepdims=True) + 1e-6)
        a[rows, :] = (wide * scale).astype(BF16)

    by_rows(a.shape[0], some)


def forward_kernel(h, w_gate, w_up, w_down, gate_out, up_out, h_out, a_t, a, total):
    step = pl.program_id(0)

    @pl.when(step == 0)
    def _():
        norm_rows(h, a)
        a_t[...] = a[...].T

    gate = dot(a[...], w_gate[0])
    up = dot(a[...], w_up[0])
    gate_out[...] = gate
    up_out[...] = up
    hidden = (gate * jax.nn.sigmoid(gate) * up).astype(BF16)
    part = dot(hidden, w_down[0])

    @pl.when(step == 0)
    def _():
        total[...] = part

    @pl.when(step > 0)
    def _():
        total[...] += part

    @pl.when(step == pl.num_programs(0) - 1)
    def _():
        def some(rows):
            h_out[0, rows, :] = (h[0, rows, :].astype(F32) + total[rows, :].astype(BF16).astype(F32)).astype(BF16)

        by_rows(a.shape[0], some)


def hidden_backward(gate, up, by_hidden):
    s = jax.nn.sigmoid(gate)
    act = gate * s
    by_hidden = by_hidden.astype(BF16).astype(F32)
    hidden = (act * up).astype(BF16)
    by_up = (by_hidden * act).astype(BF16)
    by_gate = (by_hidden * up * (s * (1 + gate * (1 - s)))).astype(BF16)
    return hidden, by_gate, by_up


def backward_kernel(h, dy, first_a_t, w_gate, w_up, w_down, first_gate, first_up, out, terms, *scratch):
    a, a_t, total, by_h, gate, up, hidden, by_gate, by_up, grads, *held = scratch
    engine = Engine(terms, out, *held)
    written = engine.written
    step = pl.program_id(0)
    last, first = step < BLOCKS, (step >= BLOCKS) & (step < 2 * BLOCKS)
    slot = step % 2

    @pl.when(step == 0)
    def _():
        engine.greet()
        norm_rows(h, a)
        a_t[...] = a[...].T

    @pl.when(step == 1)
    def _():
        engine.meet()

    def send_off(which):
        for half in range(2):
            src = grads.at[slot, which, pl.ds(half * 128, 128)]
            pltpu.make_async_copy(src, terms.at[half, pl.ds((step * 3 + which) * 128, 128)], written.at[slot]).start()

    def keep(which, value):
        rows, columns = value.shape
        for i in range(columns // 128):
            grads[slot, which, pl.ds(i * (rows // 8), rows // 8)] = value[:, i * 128 : (i + 1) * 128].reshape(rows // 8, 8, 128).astype(BF16)

    def by_down(states):
        keep(2, dot(hidden[...], states, (0, 0)))
        send_off(2)

    def by_wide(turned):
        for which, ref in ((0, by_gate), (1, by_up)):
            keep(which, dot(turned, ref[...]))
            send_off(which)

    def part(k, _):
        engine.step(jnp.where(step < BLOCKS, step * LAST_CALLS, BLOCKS * LAST_CALLS + (step - BLOCKS) * FIRST_CALLS) + k)

        @pl.when(last & (k == 0))
        def _():
            gate[...] = dot(a[...], w_gate[0])
            up[...] = dot(a[...], w_up[0])

        @pl.when(last & (k == 1))
        def _():
            hidden[...], by_gate[...], by_up[...] = hidden_backward(gate[...], up[...], dot(dy[0], w_down[0], (1, 1)))
            by_down(dy[0])

        @pl.when(last & (k == 2))
        def _():
            by_wide(a_t[...])

        @pl.when(last & (k == 3))
        def _():
            for i in range(4):
                columns = pl.ds(i * 256, 256)
                value = dot(by_gate[...], w_gate[0, columns, :], (1, 1)) + dot(by_up[...], w_up[0, columns, :], (1, 1))
                total[:, columns] = jnp.where(step == 0, value, total[:, columns] + value)

        @pl.when((step == BLOCKS - 1) & (k == 3))
        def _():
            def some(rows):
                wide = h[0, rows, :].astype(F32)
                by_a = total[rows, :].astype(BF16).astype(F32)
                scale = lax.rsqrt(jnp.mean(wide**2, -1, keepdims=True) + 1e-6)
                along = jnp.sum(by_a * wide, -1, keepdims=True)
                by_wide = by_a * scale - wide * (scale * scale * scale * along * (1.0 / a.shape[1]))
                by_h[rows, :] = (dy[0, rows, :].astype(F32) + by_wide.astype(BF16).astype(F32)).astype(BF16)

            by_rows(a.shape[0], some)

        @pl.when(first & (k == 0))
        def _():
            hidden[...], by_gate[...], by_up[...] = hidden_backward(first_gate[...], first_up[...], dot(by_h[...], w_down[0], (1, 1)))
            by_down(by_h[...])

        @pl.when(first & (k == 1))
        def _():
            by_wide(first_a_t[...])

        return 0

    calls = jnp.where(last, LAST_CALLS, jnp.where(first, FIRST_CALLS, CALLS - COMPUTE_CALLS))
    lax.fori_loop(0, calls, part, 0)

    @pl.when(step == 2 * BLOCKS)
    def _():
        engine.finish()


def summed_gradients(x, dy, w_gate, w_up, w_down):
    _, tokens, d = x.shape
    ff = w_gate.shape[2]
    assert (tokens, d, ff) == (1024, 1024, BLOCKS * BLOCK)
    once = pl.Buffered(1)
    whole = pl.BlockSpec((1, tokens, d), lambda i: (0, 0, 0), pipeline_mode=once)
    turned = pl.BlockSpec((d, tokens), lambda i: (0, 0), pipeline_mode=once)
    wide = pl.BlockSpec((1, d, BLOCK), lambda i: (0, 0, i))
    tall = pl.BlockSpec((1, BLOCK, d), lambda i: (0, i, 0))
    hidden = pl.BlockSpec((tokens, BLOCK), lambda i: (0, i))
    vmem = lambda *shape, dtype=BF16: pltpu.VMEM(shape, dtype)
    gate, up, h, a_t = pl.pallas_call(
        forward_kernel,
        out_shape=[jax.ShapeDtypeStruct((tokens, ff), F32)] * 2 + [jax.ShapeDtypeStruct(x.shape, BF16), jax.ShapeDtypeStruct((d, tokens), BF16)],
        grid=(BLOCKS,),
        in_specs=[whole, wide, wide, tall],
        out_specs=[hidden, hidden, whole, turned],
        scratch_shapes=[vmem(tokens, d), vmem(tokens, d, dtype=F32)],
        compiler_params=pltpu.CompilerParams(vmem_limit_bytes=56 * 2**20),
        name="first_layer_forward",
    )(x, w_gate, w_up, w_down)
    before = lambda i: jnp.minimum(i, BLOCKS - 1)
    after = lambda i: jnp.clip(i - BLOCKS, 0, BLOCKS - 1)
    wide = pl.BlockSpec((1, d, BLOCK), lambda i: (1, 0, before(i)))
    tall = pl.BlockSpec((1, BLOCK, d), lambda i: (jnp.where(i < BLOCKS, 1, 0), jnp.where(i < BLOCKS, before(i), after(i)), 0))
    hidden = pl.BlockSpec((tokens, BLOCK), lambda i: (0, after(i)))
    tiles = lambda *n: vmem(*n, 8, 128)
    dma = pltpu.SemaphoreType.DMA
    total = jax.ShapeDtypeStruct((2, UNITS * HALF, 8, 128), BF16)
    summed, _ = pl.pallas_call(
        backward_kernel,
        out_shape=[total, total],
        grid=(2 * BLOCKS + 1,),
        in_specs=[whole, whole, turned, wide, wide, tall, hidden, hidden],
        out_specs=[pl.BlockSpec(memory_space=pl.ANY)] * 2,
        scratch_shapes=[
            vmem(tokens, d), vmem(d, tokens), vmem(tokens, d, dtype=F32), vmem(tokens, d),
            vmem(tokens, BLOCK, dtype=F32), vmem(tokens, BLOCK, dtype=F32), vmem(tokens, BLOCK), vmem(tokens, BLOCK), vmem(tokens, BLOCK),
            tiles(2, 3, 256),
            tiles(HELD, HALF), tiles(HELD, HALF), tiles(HELD, LAY.n1), tiles(HELD, LAY.n2), tiles(HELD, LAY.n3), tiles(HELD, LAY.ns), tiles(UNITS, LAY.nf),
            dma((UNITS,)), dma((UNITS,)), dma((UNITS, LAY.sems)), dma((UNITS, 2)), dma((UNITS, 4)), dma((2,)),
            pltpu.SemaphoreType.REGULAR((UNITS - HELD,)),
        ],
        compiler_params=pltpu.CompilerParams(collective_id=0, has_side_effects=True, vmem_limit_bytes=67043328),
        name="backward_and_sum",
    )(h, dy, a_t, w_gate, w_up, w_down, gate, up)
    return summed.reshape(2, 2 * BLOCKS, 3, 128, 8, 128)


def adamw_some(w, m, v, g, new_w, new_m, new_v, at, g_at):
    g = g[g_at].astype(F32)
    one = 0.9 * m[at] + 0.1 * g
    two = 0.95 * v[at] + 0.05 * g * g
    old = w[at].astype(F32)
    step = one * lax.rsqrt(two + 1e-8) + 0.1 * old
    new_w[at] = (old - 0.02 * step).astype(BF16)
    new_m[at] = one
    new_v[at] = two


def adamw_wide_kernel(*refs):
    for column in range(2 * BLOCKS):
        adamw_some(*refs, (0, slice(None), column), (column % 2, column // 2, 0))


def adamw_tall_kernel(*refs):
    for column in range(2):
        for block in range(BLOCKS):
            adamw_some(*refs, (0, slice(block * 32, (block + 1) * 32), column), (0, block, 0, column))


def adamw(which, w, m, v, summed):
    layers, rows, columns = w.shape[:3]
    if which < 2:
        some = 32
        grid = (layers, rows // some)
        spec = pl.BlockSpec((1, some, columns, 8, 128), lambda n, i: (n, i, 0, 0, 0))
        g, g_spec = summed, pl.BlockSpec((2, BLOCKS, 1, some, 8, 128), lambda n, i: (0, 1 - n, which, i, 0, 0))
        kernel = adamw_wide_kernel
    else:
        grid = (layers, columns // 2)
        spec = pl.BlockSpec((1, rows, 2, 8, 128), lambda n, i: (n, 0, i, 0, 0))
        g = summed.reshape(2, 2 * BLOCKS, 3, 4, 32, 8, 128)
        g_spec = pl.BlockSpec((1, BLOCKS, 1, 2, 32, 8, 128), lambda n, i: (i // 2, 1 - n, which, i % 2, 0, 0, 0))
        kernel = adamw_tall_kernel
    return pl.pallas_call(
        kernel,
        out_shape=[jax.ShapeDtypeStruct(a.shape, a.dtype) for a in (w, m, v)],
        grid=grid,
        in_specs=[spec, spec, spec, g_spec],
        out_specs=[spec] * 3,
        compiler_params=pltpu.CompilerParams(vmem_limit_bytes=56 * 2**20),
        name="adamw",
    )(w, m, v, g)


def to_tiles(a):
    *lead, rows, columns = a.shape
    return jnp.swapaxes(a.reshape(*lead, rows // 8, 8, columns // 128, 128), -3, -2)


def from_tiles(t):
    *lead, rows, columns, _, _ = t.shape
    return jnp.swapaxes(t, -3, -2).reshape(*lead, rows * 8, columns * 128)


def solution(mesh):
    def step(x, dy, *arrays):
        weights, m, v = (arrays[i : i + 3] for i in (0, 3, 6))
        summed = summed_gradients(x, dy, *weights)
        new = [adamw(i, *(to_tiles(one) for one in (w, m, v)), summed) for i, (w, m, v) in enumerate(zip(weights, m, v, strict=True))]
        return tuple(from_tiles(one[which]) for which in range(3) for one in new)

    return jax.shard_map(
        step,
        mesh=mesh,
        in_specs=(P(("rep", "dp"), None, None),) * 2 + (P(None, None, None),) * 9,
        out_specs=(P("rep", None, None),) * 9,
        check_vma=False,
    )
```

```python
import jax
import jax.numpy as jnp
from jax import lax
from jax.experimental import pallas as pl
from jax.experimental.pallas import tpu as pltpu
from jax.sharding import PartitionSpec as P

MESH = pl.DeviceIdType.MESH
BF16, F32 = jnp.bfloat16, jnp.float32

BLOCK = 256
BLOCKS = 11
UNITS = 11
HALF = 768
SIZE = {"x": 4, "y": 4, "z": 8}
COLORS = []
_start = 0
_rings = [0, 2, 4, 5, 6, 7, 8, 9, 10, 12, 14]
for _axes, _slots in (("xyz", _rings), ("yxz", _rings), ("zxy", list(range(15)))):
    _n3 = 2
    _n2 = _n3 * SIZE[_axes[2]]
    _n1 = _n2 * SIZE[_axes[1]]
    COLORS.append((_axes, _start, (_n1, _n2, _n3), _slots))
    _start += _n1 * SIZE[_axes[0]]
assert _start == HALF
FIN_SLOT, SWAP_SLOT, END_SLOT = 7, 15, 16
SLOTS = 3
HELD = 7
PACE = 4
LAST_CALLS, FIRST_CALLS = 3, 2
COMPUTE_CALLS = BLOCKS * (LAST_CALLS + FIRST_CALLS)


def ready(m):
    return jnp.where(m < 5, 6 * m + 6, jnp.where(m == 5, 36, 4 * m + 16))


LAST_TURN = PACE * (END_SLOT + 1)
CALLS = COMPUTE_CALLS + LAST_TURN + 2


def begun(call):
    early = jnp.minimum(lax.div(jnp.maximum(call, 0), 6), 5)
    return jnp.where(call < 36, early, jnp.minimum(lax.div(jnp.maximum(call - 12, 0), 4), UNITS))


def ring_slots(n, hops):
    slots, at = [], 0
    for hop in range(hops):
        row = []
        for way in range(2):
            first = n - n // 2 if way == 0 else n // 2
            size = first if hop == 0 else n
            row.append((at, size))
            at += size
        slots.append(row)
    return slots, at


class Layout:
    def __init__(self):
        self.r1, self.r2, self.r3, self.s3, self.fin, self.sem = [], [], [], [], [], {}
        a1 = a2 = a3 = s3 = fin = sems = 0
        for c, (axes, _, (n1, n2, n3), _) in enumerate(COLORS):
            h1, h2, k3 = SIZE[axes[0]] // 2, SIZE[axes[1]] // 2, SIZE[axes[2]]
            slots, size = ring_slots(n1, h1)
            self.r1.append([[(a1 + s, n) for s, n in row] for row in slots])
            a1 += size
            slots, size = ring_slots(n2, h2)
            self.r2.append([[(a2 + s, n) for s, n in row] for row in slots])
            a2 += size
            self.r3.append(a3)
            a3 += (k3 - 1) * n3
            self.s3.append(s3)
            s3 += n2
            self.fin.append(fin)
            fin += n3
            for kind, count in (("r1", 2 * h1), ("r2", 2 * h2), ("r3", 1), ("g3", 1), ("g2", 2 * h2), ("g1", 2 * h1)):
                self.sem[c, kind] = sems
                sems += count
        self.n1, self.n2, self.n3, self.ns, self.nf, self.sems = a1, a2, a3, s3, fin, sems


LAY = Layout()
SENT = HALF + LAY.n1 + LAY.n2 + LAY.n3


def add_tiles(dst, dst_at, size, terms, chunk=8):
    def some(at, n):
        total = None
        for ref, start in terms:
            value = ref[pl.ds(start + at, n)].astype(F32)
            total = value if total is None else total + value
        dst[pl.ds(dst_at + at, n)] = total.astype(BF16)

    full = size // chunk
    if full > 1:
        lax.fori_loop(0, full, lambda i, _: (some(i * chunk, chunk), 0)[1], 0)
    elif full == 1:
        some(0, chunk)
    if size % chunk:
        some(full * chunk, size % chunk)


def remote(src, dst, send, receive, to):
    return pltpu.make_async_remote_copy(src_ref=src, dst_ref=dst, send_sem=send, recv_sem=receive, device_id=to, device_id_type=MESH)


def arrived(ref, n, sem):
    pltpu.make_async_copy(ref.at[pl.ds(0, n)], ref.at[pl.ds(0, n)], sem).wait()


class Engine:
    def __init__(self, terms, out, own, par, r1, r2, r3, s3, fin, send_rs, send_ag, recv, pair, load, written, credit):
        self.terms, self.out, self.own, self.par, self.r1, self.r2, self.r3, self.s3, self.fin = terms, out, own, par, r1, r2, r3, s3, fin
        self.send_rs, self.send_ag, self.recv, self.pair, self.load, self.written, self.credit = send_rs, send_ag, recv, pair, load, written, credit
        me = lax.axis_index("dp")
        self.core = lax.rem(me, 2)
        self.place = {"x": lax.div(me, 64), "y": lax.rem(lax.div(me, 16), 4), "z": lax.rem(lax.div(me, 2), 8)}
        self.peers = [self.device()] + [self.device("x", d) for d in (1, 3)]
        self.peers += [self.device("y", d) for d in (1, 2, 3)] + [self.device("z", d) for d in range(1, 8)]

    def device(self, axis=None, by=0):
        at = dict(self.place)
        core = self.core
        if axis is None:
            core = 1 - core
        else:
            at[axis] = lax.rem(at[axis] + (by + SIZE[axis]), SIZE[axis])
        return (0, ((at["x"] * 4 + at["y"]) * 8 + at["z"]) * 2 + core)

    def greet(self):
        for peer in self.peers:
            pl.semaphore_signal(pltpu.get_barrier_semaphore(), inc=1, device_id=peer, device_id_type=MESH)

    def meet(self):
        pl.semaphore_wait(pltpu.get_barrier_semaphore(), len(self.peers))

    def begin(self, m):
        for block in range(2):
            arrived(self.out.at[0], HALF, self.written.at[lax.rem(2 * m + block, SLOTS)])

        @pl.when(m >= HELD)
        def _():
            pl.semaphore_wait(self.credit.at[m - HELD], len(self.peers))
            arrived(self.out.at[0], SENT, self.send_rs.at[m - HELD])

        unit = pl.ds(m * HALF, HALF)
        pltpu.make_async_copy(self.terms.at[self.core, unit], self.own.at[lax.rem(m, HELD)], self.load.at[m, 0]).start()
        remote(self.terms.at[1 - self.core, unit], self.par.at[lax.rem(m, HELD)], self.send_rs.at[m], self.pair.at[m, 0], self.device()).start()

    def color_stage(self, c, stage, m):
        axes, start, (n1, n2, n3), _ = COLORS[c]
        k1, k2, k3 = (SIZE[a] for a in axes)
        p1, p2, p3 = (self.place[a] for a in axes)
        h1, h2 = k1 // 2, k2 // 2
        b = lax.rem(m, HELD)
        o, q, a1, a2, a3 = (ref.at[b] for ref in (self.own, self.par, self.r1, self.r2, self.r3))
        result, mine = self.out.at[self.core], m * HALF
        send_rs, send_ag, load = self.send_rs.at[m], self.send_ag.at[m], self.load.at[m, 1 + c]
        device = self.device
        base2 = start + p1 * n1
        base3 = base2 + p2 * n2
        shard = base3 + p3 * n3

        def sem(kind, i=0):
            return self.recv.at[m, LAY.sem[c, kind] + i]

        def ring_reduce(axis, k, p, n, base, hop, slots, arrivals, kind, more):
            h = k // 2
            j = h - hop
            for way, sign in ((0, 1), (1, -1)):
                owner = lax.rem(p + (sign * j + k), k)
                at = base + owner * n
                lo, size = (0, n) if j < h else ((0, n - n // 2) if way == 0 else (n - n // 2, n // 2))
                extra = [(ref, where + owner * n) for ref, where in more]
                if hop == 0:
                    add_tiles(o, at + lo, size, [(o, at + lo), (q, at + lo)] + [(r, w + lo) for r, w in extra])
                else:
                    there, got = slots[hop - 1][way]
                    arrived(arrivals, got, sem(kind, 2 * (hop - 1) + way))
                    if got == n:
                        add_tiles(o, at, n, [(o, at), (q, at)] + extra + [(arrivals, there)])
                    else:
                        first = 0 if way == 0 else n - got
                        add_tiles(o, at + first, got, [(o, at + first), (q, at + first)] + [(r, w + first) for r, w in extra] + [(arrivals, there)])
                        other, rest = (got, n - got) if way == 0 else (0, n - got)
                        add_tiles(o, at + other, rest, [(o, at + other), (q, at + other)] + [(r, w + other) for r, w in extra])
                there, size2 = slots[hop][way]
                assert size2 == size
                remote(o.at[pl.ds(at + lo, size)], arrivals.at[pl.ds(there, size)], send_rs, sem(kind, 2 * hop + way), device(axis, sign)).start()

        def ring_wait(h, slots, arrivals, kind):
            for way in range(2):
                arrived(arrivals, slots[h - 1][way][1], sem(kind, 2 * (h - 1) + way))

        def gather_sizes(k, n, hop):
            return [(0, n), (0, n)] if hop < k // 2 - 1 else [(0, n - n // 2), (n - n // 2, n // 2)]

        def gather_wait(k, n, hop, kind):
            for way in range(2):
                arrived(result, gather_sizes(k, n, hop)[way][1], sem(kind, 2 * hop + way))

        def ring_gather(axis, k, p, n, base, hop, kind):
            if hop:
                gather_wait(k, n, hop - 1, kind)
            for way, sign in ((0, 1), (1, -1)):
                lo, size = gather_sizes(k, n, hop)[way]
                piece = result.at[pl.ds(mine + base + lax.rem(p + (k - sign * hop), k) * n + lo, size)]
                remote(piece, piece, send_ag, sem(kind, 2 * hop + way), device(axis, sign)).start()

        last1 = [(a1, LAY.r1[c][h1 - 1][way][0]) for way in range(2)]
        last2 = [(a2, LAY.r2[c][h2 - 1][way][0]) for way in range(2)]
        if stage < h1:
            ring_reduce(axes[0], k1, p1, n1, start, stage, LAY.r1[c], a1, "r1", [])
            return
        stage -= h1
        if stage < h2:
            if stage == 0:
                ring_wait(h1, LAY.r1[c], a1, "r1")
            ring_reduce(axes[1], k2, p2, n2, base2, stage, LAY.r2[c], a2, "r2", last1)
            return
        stage -= h2
        if stage == 0:
            ring_wait(h2, LAY.r2[c], a2, "r2")
            add_tiles(self.s3.at[b], LAY.s3[c], n2, [(o, base3), (q, base3)] + [(r, w + p2 * n2) for r, w in last1] + last2)
            for d in range(1, k3):
                piece = self.s3.at[b, pl.ds(LAY.s3[c] + lax.rem(p3 + d, k3) * n3, n3)]
                remote(piece, a3.at[pl.ds(LAY.r3[c] + (d - 1) * n3, n3)], send_rs, sem("r3"), device(axes[2], d)).start()
            return
        stage -= 1
        if stage == 0:
            arrived(a3, (k3 - 1) * n3, sem("r3"))
            terms = [(o, shard), (q, shard)] + [(r, w + p2 * n2 + p3 * n3) for r, w in last1] + [(r, w + p3 * n3) for r, w in last2]
            terms += [(a3, LAY.r3[c] + (d - 1) * n3) for d in range(1, k3)]
            add_tiles(self.fin.at[m], LAY.fin[c], n3, terms)
            piece = self.fin.at[m, pl.ds(LAY.fin[c], n3)]
            there = result.at[pl.ds(mine + shard, n3)]
            pltpu.make_async_copy(piece, there, load).start()
            for d in range(1, k3):
                remote(piece, there, send_ag, sem("g3"), device(axes[2], d)).start()
            return
        stage -= 1
        if stage < h2:
            if stage == 0:
                arrived(result, n3, load)
                arrived(result, (k3 - 1) * n3, sem("g3"))
            ring_gather(axes[1], k2, p2, n2, base2, stage, "g2")
            return
        stage -= h2
        if stage < h1:
            if stage == 0:
                gather_wait(k2, n2, h2 - 1, "g2")
            ring_gather(axes[0], k1, p1, n1, start, stage, "g1")
            return
        gather_wait(k1, n1, h1 - 1, "g1")

    def slot(self, s, m):
        if s == -1:
            self.begin(m)
        if s == 0:
            arrived(self.out.at[0], HALF, self.load.at[m, 0])
            arrived(self.out.at[0], HALF, self.pair.at[m, 0])
        for c in (2, 0, 1):
            if s in COLORS[c][3]:
                self.color_stage(c, COLORS[c][3].index(s), m)
        if s == FIN_SLOT:

            @pl.when(m < UNITS - HELD)
            def _():
                for peer in self.peers:
                    pl.semaphore_signal(self.credit.at[m], inc=1, device_id=peer, device_id_type=MESH)

        if s == SWAP_SLOT:
            piece = self.out.at[self.core, pl.ds(m * HALF, HALF)]
            remote(piece, piece, self.send_ag.at[m], self.pair.at[m, 1], self.device()).start()
        if s == END_SLOT:
            arrived(self.out.at[0], HALF, self.pair.at[m, 1])
            arrived(self.out.at[0], SENT, self.send_ag.at[m])

    def step(self, call):
        def unit(m, _):
            since = call - ready(m)

            @pl.when(lax.rem(since, PACE) == 0)
            def _():
                s = lax.div(since, PACE) - 1
                for low in range(-1, END_SLOT + 1, 4):

                    @pl.when((s >= low) & (s < low + 4))
                    def _():
                        for one in range(low, min(low + 4, END_SLOT + 1)):
                            pl.when(s == one)(lambda one=one: self.slot(one, m))

            return 0

        lax.fori_loop(begun(call - LAST_TURN - 1), begun(call), unit, 0)

    def finish(self):
        def unit(m, _):
            arrived(self.out.at[0], SENT, self.send_rs.at[m])
            return 0

        lax.fori_loop(UNITS - HELD, UNITS, unit, 0)


def dot(a, b, contract=(1, 0)):
    return lax.dot_general(a, b, (((contract[0],), (contract[1],)), ((), ())), preferred_element_type=F32)


ROWS = 128


def by_rows(total, body):
    lax.fori_loop(0, total // ROWS, lambda i, _: (body(pl.ds(pl.multiple_of(i * ROWS, ROWS), ROWS)), 0)[1], 0)


def norm_rows(h, a):
    def some(rows):
        wide = h[0, rows, :].astype(F32)
        scale = lax.rsqrt(jnp.mean(wide**2, -1, keepdims=True) + 1e-6)
        a[rows, :] = (wide * scale).astype(BF16)

    by_rows(a.shape[0], some)


def forward_kernel(h, w_gate, w_up, w_down, gate_out, up_out, h_out, a_t, a, total):
    step = pl.program_id(0)

    @pl.when(step == 0)
    def _():
        norm_rows(h, a)
        a_t[...] = a[...].T
        total[...] = jnp.zeros_like(total)

    gate = dot(a[...], w_gate[0])
    up = dot(a[...], w_up[0])
    gate_out[...] = gate
    up_out[...] = up
    hidden = (gate * jax.nn.sigmoid(gate) * up).astype(BF16)
    for i in range(4):
        columns = slice(i * 256, (i + 1) * 256)
        total[:, columns] += dot(hidden, w_down[0, :, columns])

    @pl.when(step == pl.num_programs(0) - 1)
    def _():
        def some(rows):
            h_out[0, rows, :] = (h[0, rows, :].astype(F32) + total[rows, :].astype(BF16).astype(F32)).astype(BF16)

        by_rows(a.shape[0], some)


def hidden_backward(gate, up, by_hidden):
    s = jax.nn.sigmoid(gate)
    act = gate * s
    by_hidden = by_hidden.astype(BF16).astype(F32)
    hidden = (act * up).astype(BF16)
    by_up = (by_hidden * act).astype(BF16)
    by_gate = (by_hidden * up * (s * (1 + gate * (1 - s)))).astype(BF16)
    return hidden, by_gate, by_up


def backward_kernel(h, dy, first_a_t, w_gate, w_up, w_down, first_gate, first_up, out, terms, *scratch):
    a, a_t, total, hidden, by_gate, by_up, grads, *held = scratch
    by_h = a
    engine = Engine(terms, out, *held)
    written = engine.written
    step = pl.program_id(0)
    last, first = step < BLOCKS, (step >= BLOCKS) & (step < 2 * BLOCKS)
    slot = lax.rem(step, SLOTS)

    @pl.when(step == 0)
    def _():
        engine.greet()
        norm_rows(h, a)
        a_t[...] = a[...].T

    @pl.when(step == 1)
    def _():
        engine.meet()

    def send_off(which):
        for half in range(2):
            src = grads.at[slot, which, pl.ds(half * 128, 128)]
            pltpu.make_async_copy(src, terms.at[half, pl.ds((step * 3 + which) * 128, 128)], written.at[slot]).start()

    def keep(which, value):
        rows, columns = value.shape
        for i in range(columns // 128):
            grads[slot, which, pl.ds(i * (rows // 8), rows // 8)] = value[:, i * 128 : (i + 1) * 128].reshape(rows // 8, 8, 128).astype(BF16)

    def by_down(states):
        keep(2, dot(hidden[...], states, (0, 0)))
        send_off(2)

    def by_wide(turned):
        for which, ref in ((0, by_gate), (1, by_up)):
            keep(which, dot(turned, ref[...]))
            send_off(which)

    def part(k, _):
        engine.step(jnp.where(step < BLOCKS, step * LAST_CALLS, BLOCKS * LAST_CALLS + (step - BLOCKS) * FIRST_CALLS) + k)

        @pl.when(last & (k == 0))
        def _():
            gate, up = dot(a[...], w_gate[0]), dot(a[...], w_up[0])
            hidden[...], by_gate[...], by_up[...] = hidden_backward(gate, up, dot(dy[0], w_down[0], (1, 1)))
            by_down(dy[0])

        @pl.when(last & (k == 1))
        def _():
            by_wide(a_t[...])

        @pl.when(last & (k == 2))
        def _():
            for i in range(4):
                columns = pl.ds(i * 256, 256)
                value = dot(by_gate[...], w_gate[0, columns, :], (1, 1)) + dot(by_up[...], w_up[0, columns, :], (1, 1))
                total[:, columns] = jnp.where(step == 0, value, total[:, columns] + value)

        @pl.when((step == BLOCKS - 1) & (k == 2))
        def _():
            def some(rows):
                wide = h[0, rows, :].astype(F32)
                by_a = total[rows, :].astype(BF16).astype(F32)
                scale = lax.rsqrt(jnp.mean(wide**2, -1, keepdims=True) + 1e-6)
                along = jnp.sum(by_a * wide, -1, keepdims=True)
                by_wide = by_a * scale - wide * (scale * scale * scale * along * (1.0 / a.shape[1]))
                by_h[rows, :] = (dy[0, rows, :].astype(F32) + by_wide.astype(BF16).astype(F32)).astype(BF16)

            by_rows(a.shape[0], some)

        @pl.when(first & (k == 0))
        def _():
            hidden[...], by_gate[...], by_up[...] = hidden_backward(first_gate[...], first_up[...], dot(by_h[...], w_down[0], (1, 1)))
            by_down(by_h[...])

        @pl.when(first & (k == 1))
        def _():
            by_wide(first_a_t[...])

        return 0

    calls = jnp.where(last, LAST_CALLS, jnp.where(first, FIRST_CALLS, CALLS - COMPUTE_CALLS))
    lax.fori_loop(0, calls, part, 0)

    @pl.when(step == 2 * BLOCKS)
    def _():
        engine.finish()


def summed_gradients(x, dy, w_gate, w_up, w_down):
    _, tokens, d = x.shape
    ff = w_gate.shape[2]
    assert (tokens, d, ff) == (1024, 1024, BLOCKS * BLOCK)
    once = pl.Buffered(1)
    whole = pl.BlockSpec((1, tokens, d), lambda i: (0, 0, 0), pipeline_mode=once)
    turned = pl.BlockSpec((d, tokens), lambda i: (0, 0), pipeline_mode=once)
    wide = pl.BlockSpec((1, d, BLOCK), lambda i: (0, 0, i))
    tall = pl.BlockSpec((1, BLOCK, d), lambda i: (0, i, 0))
    hidden = pl.BlockSpec((tokens, BLOCK), lambda i: (0, i))
    vmem = lambda *shape, dtype=BF16: pltpu.VMEM(shape, dtype)
    gate, up, h, a_t = pl.pallas_call(
        forward_kernel,
        out_shape=[jax.ShapeDtypeStruct((tokens, ff), F32)] * 2 + [jax.ShapeDtypeStruct(x.shape, BF16), jax.ShapeDtypeStruct((d, tokens), BF16)],
        grid=(BLOCKS,),
        in_specs=[whole, wide, wide, tall],
        out_specs=[hidden, hidden, whole, turned],
        scratch_shapes=[vmem(tokens, d), vmem(tokens, d, dtype=F32)],
        compiler_params=pltpu.CompilerParams(vmem_limit_bytes=56 * 2**20),
        name="first_layer_forward",
    )(x, w_gate, w_up, w_down)
    before = lambda i: jnp.minimum(i, BLOCKS - 1)
    after = lambda i: jnp.clip(i - BLOCKS, 0, BLOCKS - 1)
    wide = pl.BlockSpec((1, d, BLOCK), lambda i: (1, 0, before(i)))
    tall = pl.BlockSpec((1, BLOCK, d), lambda i: (jnp.where(i < BLOCKS, 1, 0), jnp.where(i < BLOCKS, before(i), after(i)), 0))
    hidden = pl.BlockSpec((tokens, BLOCK), lambda i: (0, after(i)))
    tiles = lambda *n: vmem(*n, 8, 128)
    dma = pltpu.SemaphoreType.DMA
    total = jax.ShapeDtypeStruct((2, UNITS * HALF, 8, 128), BF16)
    summed, _ = pl.pallas_call(
        backward_kernel,
        out_shape=[total, total],
        grid=(2 * BLOCKS + 1,),
        in_specs=[whole, whole, turned, wide, wide, tall, hidden, hidden],
        out_specs=[pl.BlockSpec(memory_space=pl.ANY)] * 2,
        scratch_shapes=[
            vmem(tokens, d), vmem(d, tokens), vmem(tokens, d, dtype=F32),
            vmem(tokens, BLOCK), vmem(tokens, BLOCK), vmem(tokens, BLOCK), tiles(SLOTS, 3, 256),
            tiles(HELD, HALF), tiles(HELD, HALF), tiles(HELD, LAY.n1), tiles(HELD, LAY.n2), tiles(HELD, LAY.n3), tiles(HELD, LAY.ns), tiles(UNITS, LAY.nf),
            dma((UNITS,)), dma((UNITS,)), dma((UNITS, LAY.sems)), dma((UNITS, 2)), dma((UNITS, 4)), dma((SLOTS,)),
            pltpu.SemaphoreType.REGULAR((UNITS - HELD,)),
        ],
        compiler_params=pltpu.CompilerParams(collective_id=0, has_side_effects=True, vmem_limit_bytes=67043328),
        name="backward_and_sum",
    )(h, dy, a_t, w_gate, w_up, w_down, gate, up)
    return summed.reshape(2, 2 * BLOCKS, 3, 128, 8, 128)


def adamw_some(w, m, v, g, new_w, new_m, new_v, at, g_at):
    g = g[g_at].astype(F32)
    one = 0.9 * m[at] + 0.1 * g
    two = 0.95 * v[at] + 0.05 * g * g
    old = w[at].astype(F32)
    step = one * lax.rsqrt(two + 1e-8) + 0.1 * old
    new_w[at] = (old - 0.02 * step).astype(BF16)
    new_m[at] = one
    new_v[at] = two


def adamw_wide_kernel(*refs):
    for column in range(2 * BLOCKS):
        adamw_some(*refs, (0, slice(None), column), (column % 2, column // 2, 0))


def adamw_tall_kernel(*refs):
    for column in range(2):
        for block in range(BLOCKS):
            adamw_some(*refs, (0, slice(block * 32, (block + 1) * 32), column), (0, block, 0, column))


def adamw(which, w, m, v, summed):
    layers, rows, columns = w.shape[:3]
    if which < 2:
        some = 32
        grid = (layers, rows // some)
        spec = pl.BlockSpec((1, some, columns, 8, 128), lambda n, i: (n, i, 0, 0, 0))
        g, g_spec = summed, pl.BlockSpec((2, BLOCKS, 1, some, 8, 128), lambda n, i: (0, 1 - n, which, i, 0, 0))
        kernel = adamw_wide_kernel
    else:
        grid = (layers, columns // 2)
        spec = pl.BlockSpec((1, rows, 2, 8, 128), lambda n, i: (n, 0, i, 0, 0))
        g = summed.reshape(2, 2 * BLOCKS, 3, 4, 32, 8, 128)
        g_spec = pl.BlockSpec((1, BLOCKS, 1, 2, 32, 8, 128), lambda n, i: (i // 2, 1 - n, which, i % 2, 0, 0, 0))
        kernel = adamw_tall_kernel
    return pl.pallas_call(
        kernel,
        out_shape=[jax.ShapeDtypeStruct(a.shape, a.dtype) for a in (w, m, v)],
        grid=grid,
        in_specs=[spec, spec, spec, g_spec],
        out_specs=[spec] * 3,
        compiler_params=pltpu.CompilerParams(vmem_limit_bytes=56 * 2**20),
        name="adamw",
    )(w, m, v, g)


def to_tiles(a):
    *lead, rows, columns = a.shape
    return jnp.swapaxes(a.reshape(*lead, rows // 8, 8, columns // 128, 128), -3, -2)


def from_tiles(t):
    *lead, rows, columns, _, _ = t.shape
    return jnp.swapaxes(t, -3, -2).reshape(*lead, rows * 8, columns * 128)


def solution(mesh):
    def step(x, dy, *arrays):
        weights, m, v = (arrays[i : i + 3] for i in (0, 3, 6))
        summed = summed_gradients(x, dy, *weights)
        new = [adamw(i, *(to_tiles(one) for one in (w, m, v)), summed) for i, (w, m, v) in enumerate(zip(weights, m, v, strict=True))]
        return tuple(from_tiles(one[which]) for which in range(3) for one in new)

    return jax.shard_map(
        step,
        mesh=mesh,
        in_specs=(P(("rep", "dp"), None, None),) * 2 + (P(None, None, None),) * 9,
        out_specs=(P("rep", None, None),) * 9,
        check_vma=False,
    )
```
